32 devices in a mesh: batch: 4 (over y, x), mp: 8 (over z, core).
Axes of the slice: x: 2, y: 2, z: 4, core: 2. Of those that a mesh axis runs over, the one named last changes fastest.
Arguments:
- queries: bfloat16 [8192, 768], P(('batch', 'mp')), may hold values from -2 to 2
- docs: bfloat16 [8192, 768], P(('batch', 'mp')), may hold values from -2 to 2
- doc_id: int32 [8192], P(('batch', 'mp')), may hold values from 0 to 4095, as said below
- owner_row: int32 [4096], P(('batch', 'mp')), may hold values from 0 to 4095, as said below
Outputs:
- query_grad: bfloat16 [8192, 768], P(('batch', 'mp'))
- doc_grad: bfloat16 [4096, 768], P(('batch', 'mp'))
- loss: float32 [], replicated
The draws below stay inside these ranges and needn't reach their ends.
Inputs may be any that keep to these rules, and one draw needn't show every extreme that they name: `doc_id`: pairs may share a document; document u is held by block u // 128 of the table; the pairs of a device name documents of blocks of its own batch index only; no more than 64 pairs of one device name documents of one block, and on every device some block is named by exactly 64 of its pairs. `owner_row`: distinct rows; the row of document u lies in rows (u // 128) * 128 to (u // 128) * 128 + 127.
All inputs are finite; a program needn't handle non-finite values.
Results may differ from the reference program's by a relative error of at most 0.003.
Values may be sent and summed in bfloat16 or wider, within the bound.
A program may use at most 64 MiB of HBM per device.

```python
import jax
import jax.numpy as jnp
from jax import lax

D = 768
ROWS = 256
OWN_ROWS = 128
GROUP = 1024
PAIRS = 8192
TABLE = 4096
SLOTS = 64
N_BATCH = 4
N_MP = 8


def pair_tower(key):
    first, second = jax.random.split(jax.random.fold_in(key, 7), 2)
    scale = D ** (-0.5)
    query_rows = jax.random.normal(first, (PAIRS, D), jnp.float32) * scale
    doc_rows = jax.random.normal(second, (PAIRS, D), jnp.float32) * scale
    device_pos = (jnp.arange(PAIRS, dtype=jnp.int32) // ROWS).astype(jnp.float32) / (N_BATCH * N_MP - 1)
    ramp = jnp.exp(jnp.log(0.3) + (jnp.log(3.0) - jnp.log(0.3)) * device_pos)[:, None]
    query_rows = query_rows * ramp
    return (jnp.clip(query_rows, -2.0, 2.0), jnp.clip(doc_rows, -2.0, 2.0))


def draw_queries(key, part):
    return pair_tower(key)[0].astype(jnp.bfloat16)


def draw_docs(key, part):
    return pair_tower(key)[1].astype(jnp.bfloat16)


def block_owners(block_key):
    first, second, third = jax.random.split(block_key, 3)
    chosen = jax.random.randint(first, (), 0, N_MP)
    shuffled = jax.random.permutation(second, N_MP * SLOTS).astype(jnp.int32)
    priority = jnp.where(shuffled // SLOTS == chosen, 0, 1).astype(jnp.int32)
    order = jnp.argsort(priority, stable=True)
    taken = shuffled[order][:ROWS]
    return (jax.random.permutation(third, taken) // SLOTS).astype(jnp.int32)


def draw_doc_id(key, part):
    first, second, third = jax.random.split(jax.random.fold_in(key, 13), 3)
    blocks = N_BATCH * N_MP
    columns = jax.vmap(block_owners)(jax.random.split(first, blocks)).reshape(PAIRS)
    left = jax.random.randint(second, (PAIRS,), 0, OWN_ROWS)
    right = jax.random.randint(third, (PAIRS,), 0, OWN_ROWS)
    local = left * right // OWN_ROWS
    batch_row = jnp.arange(PAIRS, dtype=jnp.int32) // (ROWS * N_MP)
    return ((batch_row * N_MP + columns) * OWN_ROWS + local).astype(jnp.int32)


def draw_owner_row(key, part):
    blocks = N_BATCH * N_MP
    keys = jax.random.split(jax.random.fold_in(key, 17), blocks)
    shuffled = jax.vmap(lambda one: jax.random.permutation(one, OWN_ROWS).astype(jnp.int32))(keys)
    base = jnp.arange(blocks, dtype=jnp.int32)[:, None] * OWN_ROWS
    return (shuffled + base).reshape(TABLE).astype(jnp.int32)


def setup_inputs(seed: int = 0) -> dict:
    key_of = jax.random.split(jax.random.key(seed), 5)
    queries = draw_queries(jax.random.fold_in(key_of[4], 71), 0)
    docs = draw_docs(jax.random.fold_in(key_of[4], 71), 0)
    doc_id = draw_doc_id(jax.random.fold_in(key_of[4], 71), 0)
    owner_row = draw_owner_row(jax.random.fold_in(key_of[4], 71), 0)
    return {"queries": queries, "docs": docs, "doc_id": doc_id, "owner_row": owner_row}


inverse_temp = 80.0


def group_backward(q_group, d_group):
    scores = jnp.dot(q_group, d_group.T, preferred_element_type=jnp.float32) * inverse_temp
    row_max = jnp.max(scores, axis=1, keepdims=True)
    exp_terms = jnp.exp(scores - row_max)
    row_total = jnp.sum(exp_terms, axis=1, keepdims=True)
    prob = exp_terms / row_total
    own_mask = jnp.eye(GROUP, dtype=scores.dtype)
    loss_part = jnp.sum(row_max[:, 0] + jnp.log(row_total[:, 0]) - jnp.diagonal(scores))
    grad_scores = (prob - own_mask).astype(jnp.bfloat16)
    query_part = (jnp.dot(grad_scores, d_group, preferred_element_type=jnp.float32) * inverse_temp).astype(jnp.bfloat16)
    pair_part = jnp.dot(grad_scores.T, q_group, preferred_element_type=jnp.float32) * inverse_temp
    return query_part, pair_part, loss_part


def to_groups(values):
    return values.reshape(N_BATCH, N_MP, ROWS, D).transpose(1, 0, 2, 3).reshape(N_MP, GROUP, D)


def from_groups(values):
    return values.reshape(N_MP, N_BATCH, ROWS, D).transpose(1, 0, 2, 3).reshape(PAIRS, D)


def reference(queries, docs, doc_id, owner_row):
    query_parts, pair_parts, losses = lax.map(lambda pair: group_backward(pair[0], pair[1]), (to_groups(queries), to_groups(docs)))
    query_grad = from_groups(query_parts)
    pair_grad = from_groups(pair_parts)
    loss = jnp.sum(losses) / PAIRS
    table_rows = owner_row[doc_id].astype(jnp.int32)
    doc_grad = jnp.zeros((TABLE, D), pair_grad.dtype).at[table_rows].add(pair_grad).astype(jnp.bfloat16)
    return query_grad, doc_grad, loss
```

```python
import functools

import jax
import jax.numpy as jnp
from jax import lax
from jax.experimental import pallas as pl
from jax.experimental.pallas import tpu as pltpu
from jax.sharding import PartitionSpec as P

inverse_temp = 80.0
f32 = jnp.float32
bf16 = jnp.bfloat16
NT = (((1,), (1,)), ((), ()))
NN = (((1,), (0,)), ((), ()))
TN = (((0,), (0,)), ((), ()))


def dot(x, y, dims=NN):
    return lax.dot_general(x, y, dims, preferred_element_type=f32)


def iota(shape, dim):
    return lax.broadcasted_iota(jnp.int32, shape, dim)


def send(src, dst, send_sem, recv_sem, device):
    pltpu.make_async_remote_copy(
        src_ref=src,
        dst_ref=dst,
        send_sem=send_sem,
        recv_sem=recv_sem,
        device_id=device,
        device_id_type=pl.DeviceIdType.MESH,
    ).start()


def wait(ref, sem):
    pltpu.make_async_copy(ref, ref, sem).wait()


def kernel(
    n_a, n_b, n_mp, slots, n_ch,
    q_ref, d_ref, id_ref, own_ref,
    qg_ref, dg_ref, loss_ref,
    qbuf, dbuf, st, gt, stat_own, stat_buf,
    qg_send, qg_buf, pg_send, pg_buf, zsend, zbuf,
    ids_buf, place_t, place, pick, loss_b, loss_m, loss_own, loss_grp,
    q_ss, q_rs, d_ss, d_rs, s_ss, s_rs, qg_ss, qg_rs, pg_ss, pg_rs,
    z_ss, z_rs, id_ss, id_rs, l_ss, l_rs,
):
    rows, width = q_ref.shape
    own_rows = own_ref.shape[1]
    cw = width // n_ch
    n_batch = n_a * n_b
    me_b = lax.axis_index("batch")
    me_m = lax.axis_index("mp")
    a = me_b // n_b
    c = me_b % n_b

    def row_peer(j):
        return {"batch": a * n_b + (c + j) % n_b, "mp": me_m}

    def col_peer(i):
        return {"batch": ((a + i) % n_a) * n_b + c, "mp": me_m}

    def batch_peer(t):
        return {"batch": (me_b + t) % n_batch, "mp": me_m}

    def mp_peer(k):
        return {"batch": me_b, "mp": (me_m + k) % n_mp}

    barrier = pltpu.get_barrier_semaphore()
    for t in range(1, n_batch):
        pl.semaphore_signal(
            barrier, inc=1, device_id=batch_peer(t), device_id_type=pl.DeviceIdType.MESH
        )
    for k in range(1, n_mp):
        pl.semaphore_signal(
            barrier, inc=1, device_id=mp_peer(k), device_id_type=pl.DeviceIdType.MESH
        )
    pl.semaphore_wait(barrier, n_batch + n_mp - 2)

    for j in range(1, n_b):
        to = n_b - j - 1
        send(q_ref, qbuf.at[to], q_ss.at[j - 1], q_rs.at[to], row_peer(j))
    for i in range(1, n_a):
        to = n_a - i - 1
        send(d_ref, dbuf.at[to], d_ss.at[i - 1], d_rs.at[to], col_peer(i))
    for k in range(1, n_mp):
        send(id_ref, ids_buf.at[k - 1], id_ss, id_rs, mp_peer(k))

    eye = iota((rows, rows), 0) == iota((rows, rows), 1)
    s00 = dot(d_ref[...], q_ref[...], NT) * inverse_temp
    st[0, 0] = s00
    own_score = jnp.sum(jnp.where(eye, s00, 0.0), axis=0, keepdims=True)

    upper = (iota((rows, rows), 0) < iota((rows, rows), 1)).astype(bf16)
    which = iota((n_mp, rows), 0)
    col = me_m + which
    col = jnp.where(col >= n_mp, col - n_mp, col)
    first = (me_b * n_mp + col) * own_rows
    ids = jnp.broadcast_to(id_ref[...], (n_mp, rows))
    mask = ((ids >= first) & (ids < first + own_rows)).astype(f32)
    rank = dot(mask.astype(bf16), upper)
    slot = jnp.sum(mask * (rank + (which * slots).astype(f32)), axis=0, keepdims=True)
    slot = slot.astype(jnp.int32)
    pick[...] = (iota((n_mp * slots, rows), 0) == slot).astype(f32).astype(bf16)

    base = (me_b * n_mp + me_m) * own_rows
    owner = (iota((own_rows, own_rows), 0) == own_ref[...] - base).astype(f32).astype(bf16)

    def place_block(k, ids_k):
        local = ids_k - base
        here = ((local >= 0) & (local < own_rows)).astype(f32)
        doc = (iota((own_rows, rows), 0) == local).astype(f32).astype(bf16)
        target = dot(owner, doc).astype(bf16)
        rank_k = dot(jnp.broadcast_to(here, (8, rows)).astype(bf16), upper)[0:1]
        rank_k = jnp.where(here > 0.0, rank_k, -1.0).astype(jnp.int32)
        taken = (iota((slots, rows), 0) == rank_k).astype(f32).astype(bf16)
        place_t[pl.ds(k * slots, slots), :] = dot(taken, target, NT)

    place_block(0, id_ref[...])
    wait(ids_buf, id_rs)
    for k in range(1, n_mp):
        place_block(k, ids_buf[k - 1])
    place[...] = jnp.transpose(place_t[...]).astype(bf16)

    def q_of(j):
        return q_ref if j == 0 else qbuf.at[j - 1]

    def d_of(i):
        return d_ref if i == 0 else dbuf.at[i - 1]

    for i in range(1, n_a):
        wait(dbuf.at[i - 1], d_rs.at[i - 1])
        st[i, 0] = dot(d_of(i)[...], q_ref[...], NT) * inverse_temp
    for j in range(1, n_b):
        wait(qbuf.at[j - 1], q_rs.at[j - 1])
        for i in range(n_a):
            st[i, j] = dot(d_of(i)[...], q_of(j)[...], NT) * inverse_temp

    for j in range(n_b):
        top = jnp.max(st[0, j], axis=0, keepdims=True)
        for i in range(1, n_a):
            top = jnp.maximum(top, jnp.max(st[i, j], axis=0, keepdims=True))
        total = jnp.zeros_like(top)
        for i in range(n_a):
            e = jnp.exp(st[i, j] - top)
            st[i, j] = e
            total = total + jnp.sum(e, axis=0, keepdims=True)
        stat_own[pl.ds(2 * j, 1), :] = top
        stat_own[pl.ds(2 * j + 1, 1), :] = total
    for j in range(1, n_b):
        to = n_b - j - 1
        send(stat_own, stat_buf.at[to], s_ss.at[j - 1], s_rs.at[to], row_peer(j))
    for j in range(1, n_b):
        wait(stat_buf.at[j - 1], s_rs.at[j - 1])

    for j in range(n_b):
        tops = [stat_own[pl.ds(2 * j, 1), :]]
        totals = [stat_own[pl.ds(2 * j + 1, 1), :]]
        for s in range(1, n_b):
            r = (j - s) % n_b
            tops.append(stat_buf[s - 1, pl.ds(2 * r, 1), :])
            totals.append(stat_buf[s - 1, pl.ds(2 * r + 1, 1), :])
        top = functools.reduce(jnp.maximum, tops)
        total = sum(t * jnp.exp(m - top) for m, t in zip(tops, totals))
        scale = jnp.exp(tops[0] - top) / total
        if j == 0:
            part = jnp.sum(top + jnp.log(total) - own_score, axis=1, keepdims=True)
            loss_own[...] = jnp.broadcast_to(part, loss_own.shape)
        for i in range(n_a):
            p = st[i, j] * scale
            if i == 0 and j == 0:
                p = p - eye.astype(f32)
            gt[i, j] = p.astype(bf16)

    def pair_part(i, ch):
        at = pl.ds(ch * cw, cw)
        return sum(dot(gt[i, j], q_of(j)[:, at]) for j in range(n_b)) * inverse_temp

    def query_part(j):
        return sum(dot(gt[i, j], d_of(i)[...], TN) for i in range(n_a)) * inverse_temp

    for ch in range(n_ch):
        for i in range(1, n_a):
            to = n_a - i - 1
            pg_send[i - 1, ch] = pair_part(i, ch).astype(bf16)
            send(
                pg_send.at[i - 1, ch], pg_buf.at[to, ch],
                pg_ss.at[i - 1, ch], pg_rs.at[to, ch], col_peer(i),
            )
    for j in range(1, n_b):
        to = n_b - j - 1
        qg_send[j - 1] = query_part(j).astype(bf16)
        send(qg_send.at[j - 1], qg_buf.at[to], qg_ss.at[j - 1], qg_rs.at[to], row_peer(j))

    for t in range(1, n_batch):
        send(loss_own, loss_b.at[me_b], l_ss.at[0], l_rs.at[0], batch_peer(t))
    loss_b[me_b] = loss_own[...]

    for ch in range(n_ch):
        part = pair_part(0, ch)
        for i in range(1, n_a):
            wait(pg_buf.at[i - 1, ch], pg_rs.at[i - 1, ch])
            part = part + pg_buf[i - 1, ch].astype(f32)
        zsend[ch] = dot(pick[...], part.astype(bf16)).astype(bf16)
        for k in range(1, n_mp):
            at = pl.ds(k * slots, slots)
            send(zsend.at[ch, at], zbuf.at[ch, at], z_ss.at[ch], z_rs.at[ch], mp_peer(k))
        zbuf[ch, pl.ds(0, slots)] = zsend[ch, pl.ds(0, slots)]

    wait(loss_b.at[pl.ds(0, n_batch - 1)], l_rs.at[0])
    loss_grp[...] = jnp.sum(loss_b[...], axis=0)
    for k in range(1, n_mp):
        send(loss_grp, loss_m.at[me_m], l_ss.at[1], l_rs.at[1], mp_peer(k))
    loss_m[me_m] = loss_grp[...]

    grad = query_part(0)
    for j in range(1, n_b):
        wait(qg_buf.at[j - 1], qg_rs.at[j - 1])
        grad = grad + qg_buf[j - 1].astype(f32)
    qg_ref[...] = grad.astype(bf16)

    wait(loss_m.at[pl.ds(0, n_mp - 1)], l_rs.at[1])
    loss_sum = jnp.sum(loss_m[...], axis=0)
    loss_ref[0, 0] = jnp.max(loss_sum) / (rows * n_batch * n_mp)

    for ch in range(n_ch):
        wait(zbuf.at[ch, pl.ds(slots, (n_mp - 1) * slots)], z_rs.at[ch])
        dg_ref[:, pl.ds(ch * cw, cw)] = dot(place[...], zbuf[ch]).astype(bf16)

    for j in range(1, n_b):
        wait(q_ref, q_ss.at[j - 1])
        wait(stat_own, s_ss.at[j - 1])
        wait(qg_send.at[j - 1], qg_ss.at[j - 1])
    for i in range(1, n_a):
        wait(d_ref, d_ss.at[i - 1])
        for ch in range(n_ch):
            wait(pg_send.at[i - 1, ch], pg_ss.at[i - 1, ch])
    wait(ids_buf, id_ss)
    for ch in range(n_ch):
        wait(zsend.at[ch, pl.ds(slots, (n_mp - 1) * slots)], z_ss.at[ch])
    wait(loss_b.at[pl.ds(0, n_batch - 1)], l_ss.at[0])
    wait(loss_m.at[pl.ds(0, n_mp - 1)], l_ss.at[1])


def per_device(n_batch, n_mp, queries, docs, doc_id, owner_row):
    rows, width = queries.shape
    own_rows = owner_row.shape[0]
    n_a = next(x for x in range(1, n_batch + 1) if n_batch % x == 0 and x * x >= n_batch)
    n_b = n_batch // n_a
    slots = max(16, -(-2 * rows // n_mp // 16) * 16)
    n_ch = 3
    cw = width // n_ch
    vmem = pl.BlockSpec(memory_space=pltpu.VMEM)
    dma = pltpu.SemaphoreType.DMA
    ra, rb = max(n_a - 1, 1), max(n_b - 1, 1)
    query_grad, doc_grad, loss = pl.pallas_call(
        functools.partial(kernel, n_a, n_b, n_mp, slots, n_ch),
        out_shape=(
            jax.ShapeDtypeStruct((rows, width), bf16),
            jax.ShapeDtypeStruct((own_rows, width), bf16),
            jax.ShapeDtypeStruct((1, 1), f32),
        ),
        in_specs=[vmem] * 4,
        out_specs=(vmem, vmem, pl.BlockSpec(memory_space=pltpu.SMEM)),
        scratch_shapes=[
            pltpu.VMEM((rb, rows, width), bf16),
            pltpu.VMEM((ra, rows, width), bf16),
            pltpu.VMEM((n_a, n_b, rows, rows), f32),
            pltpu.VMEM((n_a, n_b, rows, rows), bf16),
            pltpu.VMEM((2 * n_b, rows), f32),
            pltpu.VMEM((rb, 2 * n_b, rows), f32),
            pltpu.VMEM((rb, rows, width), bf16),
            pltpu.VMEM((rb, rows, width), bf16),
            pltpu.VMEM((ra, n_ch, rows, cw), bf16),
            pltpu.VMEM((ra, n_ch, rows, cw), bf16),
            pltpu.VMEM((n_ch, n_mp * slots, cw), bf16),
            pltpu.VMEM((n_ch, n_mp * slots, cw), bf16),
            pltpu.VMEM((n_mp - 1, 1, rows), jnp.int32),
            pltpu.VMEM((n_mp * slots, own_rows), f32),
            pltpu.VMEM((own_rows, n_mp * slots), bf16),
            pltpu.VMEM((n_mp * slots, rows), bf16),
            pltpu.VMEM((n_batch, 1, 128), f32),
            pltpu.VMEM((n_mp, 1, 128), f32),
            pltpu.VMEM((1, 128), f32),
            pltpu.VMEM((1, 128), f32),
            dma((rb,)), dma((rb,)), dma((ra,)), dma((ra,)), dma((rb,)), dma((rb,)),
            dma((rb,)), dma((rb,)), dma((ra, n_ch)), dma((ra, n_ch)),
            dma((n_ch,)), dma((n_ch,)), dma, dma, dma((2,)), dma((2,)),
        ],
        compiler_params=pltpu.CompilerParams(
            collective_id=0, has_side_effects=True, vmem_limit_bytes=60000 * 1024
        ),
    )(queries, docs, doc_id.reshape(1, rows), owner_row.reshape(1, own_rows))
    return query_grad, doc_grad, loss.reshape(())


def solution(mesh):
    in_specs = (
        P(("batch", "mp"), None),
        P(("batch", "mp"), None),
        P(("batch", "mp")),
        P(("batch", "mp")),
    )
    out_specs = (P(("batch", "mp"), None), P(("batch", "mp"), None), P())
    body = functools.partial(per_device, mesh.shape["batch"], mesh.shape["mp"])
    return jax.shard_map(
        body, mesh=mesh, in_specs=in_specs, out_specs=out_specs, check_vma=False
    )
```

```python
import functools

import jax
import jax.numpy as jnp
from jax import lax
from jax.experimental import pallas as pl
from jax.experimental.pallas import tpu as pltpu
from jax.sharding import PartitionSpec as P

inverse_temp = 80.0
f32 = jnp.float32
bf16 = jnp.bfloat16
NT = (((1,), (1,)), ((), ()))
NN = (((1,), (0,)), ((), ()))
TN = (((0,), (0,)), ((), ()))


def dot(x, y, dims=NN):
    return lax.dot_general(x, y, dims, preferred_element_type=f32)


def iota(shape, dim):
    return lax.broadcasted_iota(jnp.int32, shape, dim)


def send(src, dst, send_sem, recv_sem, device):
    pltpu.make_async_remote_copy(
        src_ref=src,
        dst_ref=dst,
        send_sem=send_sem,
        recv_sem=recv_sem,
        device_id=device,
        device_id_type=pl.DeviceIdType.MESH,
    ).start()


def partner(m, k, n):
    if n & (n - 1):
        return (m + k) % n
    bit = 1
    while bit < n:
        if k & bit:
            m = m + bit * (1 - 2 * ((m // bit) % 2))
        bit *= 2
    return m


def wait(ref, sem):
    pltpu.make_async_copy(ref, ref, sem).wait()


def kernel(
    n_a, n_b, n_mp, slots, n_ch,
    q_hbm, d_hbm, id_hbm, own_hbm,
    qg_ref, dg_ref, loss_ref,
    qbuf, dbuf, st, gt, stat_own, stat_buf,
    qg_send, qg_buf, pg_send, pg_buf, zsend, zbuf,
    ids_buf, place_t, place, pick, loss_b, loss_m, loss_own, loss_grp,
    q_ref, d_ref, id_ref, own_ref,
    q_ss, q_rs, d_ss, d_rs, s_ss, s_rs, qg_ss, qg_rs, pg_ss, pg_rs,
    z_ss, z_rs, id_ss, id_rs, l_ss, l_rs, in_sem,
):
    rows, width = q_ref.shape
    own_rows = own_ref.shape[1]
    cw = width // n_ch
    n_batch = n_a * n_b
    me_b = lax.axis_index("batch")
    me_m = lax.axis_index("mp")
    a = me_b // n_b
    c = me_b % n_b

    def row_peer(j):
        return {"batch": a * n_b + (c + j) % n_b, "mp": me_m}

    def col_peer(i):
        return {"batch": ((a + i) % n_a) * n_b + c, "mp": me_m}

    def batch_peer(t):
        return {"batch": (me_b + t) % n_batch, "mp": me_m}

    def mp_peer(k):
        return {"batch": me_b, "mp": partner(me_m, k, n_mp)}

    load_q = pltpu.make_async_copy(q_hbm, q_ref, in_sem.at[0])
    load_d = pltpu.make_async_copy(d_hbm, d_ref, in_sem.at[1])
    load_id = pltpu.make_async_copy(id_hbm, id_ref, in_sem.at[2])
    load_own = pltpu.make_async_copy(own_hbm, own_ref, in_sem.at[3])
    loads = (load_q, load_d, load_id, load_own)
    for load in loads:
        load.start()

    barrier = pltpu.get_barrier_semaphore()
    for t in range(1, n_batch):
        pl.semaphore_signal(
            barrier, inc=1, device_id=batch_peer(t), device_id_type=pl.DeviceIdType.MESH
        )
    for k in range(1, n_mp):
        pl.semaphore_signal(
            barrier, inc=1, device_id=mp_peer(k), device_id_type=pl.DeviceIdType.MESH
        )
    pl.semaphore_wait(barrier, n_batch + n_mp - 2)
    for load in loads:
        load.wait()

    for j in range(1, n_b):
        to = n_b - j - 1
        send(q_ref, qbuf.at[to], q_ss.at[j - 1], q_rs.at[to], row_peer(j))
    for i in range(1, n_a):
        to = n_a - i - 1
        send(d_ref, dbuf.at[to], d_ss.at[i - 1], d_rs.at[to], col_peer(i))
    for k in range(1, n_mp):
        send(id_ref, ids_buf.at[k - 1], id_ss, id_rs, mp_peer(k))

    eye = iota((rows, rows), 0) == iota((rows, rows), 1)
    s00 = dot(d_ref[...], q_ref[...], NT) * inverse_temp
    st[0, 0] = s00
    own_score = jnp.sum(jnp.where(eye, s00, 0.0), axis=0, keepdims=True)

    upper = (iota((rows, rows), 0) < iota((rows, rows), 1)).astype(bf16)
    which = iota((n_mp, rows), 0)
    if n_mp & (n_mp - 1):
        col = me_m + which
        col = jnp.where(col >= n_mp, col - n_mp, col)
    else:
        col = jnp.broadcast_to(me_m, which.shape) ^ which
    first = (me_b * n_mp + col) * own_rows
    ids = jnp.broadcast_to(id_ref[...], (n_mp, rows))
    mask = ((ids >= first) & (ids < first + own_rows)).astype(f32)
    rank = dot(mask.astype(bf16), upper)
    count = jnp.sum(mask, axis=1, keepdims=True)
    first_slot = (which * slots).astype(f32)
    slot = jnp.sum(mask * (rank + first_slot), axis=0, keepdims=True)
    free = mask * (rank + count < slots).astype(f32)
    spare = jnp.sum(free * (rank + count + first_slot + 1.0), axis=0, keepdims=True) - 1.0
    at = iota((n_mp * slots, rows), 0)
    pick[:, pl.ds(0, rows)] = (at == slot.astype(jnp.int32)).astype(f32).astype(bf16)
    pick[:, pl.ds(rows, rows)] = (at == spare.astype(jnp.int32)).astype(f32).astype(bf16)

    base = (me_b * n_mp + me_m) * own_rows
    owner = (iota((own_rows, own_rows), 0) == own_ref[...] - base).astype(f32).astype(bf16)

    def place_block(k, ids_k):
        local = ids_k - base
        here = ((local >= 0) & (local < own_rows)).astype(f32)
        doc = (iota((own_rows, rows), 0) == local).astype(f32).astype(bf16)
        target = dot(owner, doc).astype(bf16)
        rank_k = dot(jnp.broadcast_to(here, (8, rows)).astype(bf16), upper)[0:1]
        spare_k = rank_k + jnp.sum(here, axis=1, keepdims=True)
        rank_k = jnp.where(here > 0.0, rank_k, -1.0).astype(jnp.int32)
        spare_k = jnp.where(here > 0.0, spare_k, -1.0).astype(jnp.int32)
        at_k = iota((slots, rows), 0)
        taken = ((at_k == rank_k) | (at_k == spare_k)).astype(f32).astype(bf16)
        place_t[pl.ds(k * slots, slots), :] = dot(taken, target, NT)

    place_block(0, id_ref[...])
    wait(ids_buf, id_rs)
    for k in range(1, n_mp):
        place_block(k, ids_buf[k - 1])
    place[...] = jnp.transpose(place_t[...]).astype(bf16)

    def q_of(j):
        return q_ref if j == 0 else qbuf.at[j - 1]

    def d_of(i):
        return d_ref if i == 0 else dbuf.at[i - 1]

    for i in range(1, n_a):
        wait(dbuf.at[i - 1], d_rs.at[i - 1])
        st[i, 0] = dot(d_of(i)[...], q_ref[...], NT) * inverse_temp
    for j in range(1, n_b):
        wait(qbuf.at[j - 1], q_rs.at[j - 1])
        for i in range(n_a):
            st[i, j] = dot(d_of(i)[...], q_of(j)[...], NT) * inverse_temp

    for j in range(n_b):
        top = jnp.max(st[0, j], axis=0, keepdims=True)
        for i in range(1, n_a):
            top = jnp.maximum(top, jnp.max(st[i, j], axis=0, keepdims=True))
        total = jnp.zeros_like(top)
        for i in range(n_a):
            e = jnp.exp(st[i, j] - top)
            st[i, j] = e
            total = total + jnp.sum(e, axis=0, keepdims=True)
        stat_own[pl.ds(2 * j, 1), :] = top
        stat_own[pl.ds(2 * j + 1, 1), :] = total
    for j in range(1, n_b):
        to = n_b - j - 1
        send(stat_own, stat_buf.at[to], s_ss.at[j - 1], s_rs.at[to], row_peer(j))
    for j in range(1, n_b):
        wait(stat_buf.at[j - 1], s_rs.at[j - 1])

    for j in range(n_b):
        tops = [stat_own[pl.ds(2 * j, 1), :]]
        totals = [stat_own[pl.ds(2 * j + 1, 1), :]]
        for s in range(1, n_b):
            r = (j - s) % n_b
            tops.append(stat_buf[s - 1, pl.ds(2 * r, 1), :])
            totals.append(stat_buf[s - 1, pl.ds(2 * r + 1, 1), :])
        top = functools.reduce(jnp.maximum, tops)
        total = sum(t * jnp.exp(m - top) for m, t in zip(tops, totals))
        scale = jnp.exp(tops[0] - top) / total
        if j == 0:
            part = jnp.sum(top + jnp.log(total) - own_score, axis=1, keepdims=True)
            loss_own[...] = jnp.broadcast_to(part, loss_own.shape)
            loss_b[me_b] = loss_own[...]
            for t in range(1, n_batch):
                send(loss_own, loss_b.at[me_b], l_ss.at[0], l_rs.at[0], batch_peer(t))
        for i in range(n_a):
            p = st[i, j] * scale
            if i == 0 and j == 0:
                p = p - eye.astype(f32)
            gt[i, j] = p.astype(bf16)

    def pair_part(i, ch):
        at = pl.ds(ch * cw, cw)
        return sum(dot(gt[i, j], q_of(j)[:, at]) for j in range(n_b)) * inverse_temp

    def query_part(j):
        return sum(dot(gt[i, j], d_of(i)[...], TN) for i in range(n_a)) * inverse_temp

    for ch in range(n_ch):
        for i in range(1, n_a):
            to = n_a - i - 1
            pg_send[i - 1, ch] = pair_part(i, ch).astype(bf16)
            send(
                pg_send.at[i - 1, ch], pg_buf.at[to, ch],
                pg_ss.at[i - 1, ch], pg_rs.at[to, ch], col_peer(i),
            )
    for j in range(1, n_b):
        to = n_b - j - 1
        qg_send[j - 1] = query_part(j).astype(bf16)
        send(qg_send.at[j - 1], qg_buf.at[to], qg_ss.at[j - 1], qg_rs.at[to], row_peer(j))

    wait(loss_b.at[pl.ds(0, n_batch - 1)], l_rs.at[0])
    loss_grp[...] = jnp.sum(loss_b[...], axis=0)
    for k in range(1, n_mp):
        send(loss_grp, loss_m.at[me_m], l_ss.at[1], l_rs.at[1], mp_peer(k))
    loss_m[me_m] = loss_grp[...]

    for ch in range(n_ch):
        part = pair_part(0, ch)
        for i in range(1, n_a):
            wait(pg_buf.at[i - 1, ch], pg_rs.at[i - 1, ch])
            part = part + pg_buf[i - 1, ch].astype(f32)
        high = part.astype(bf16)
        low = (part - high.astype(f32)).astype(bf16)
        zsend[ch] = dot(pick[...], jnp.concatenate([high, low], axis=0)).astype(bf16)
        for k in reversed(range(1, n_mp)):
            at = pl.ds(k * slots, slots)
            send(zsend.at[ch, at], zbuf.at[ch, at], z_ss.at[ch], z_rs.at[ch], mp_peer(k))
        zbuf[ch, pl.ds(0, slots)] = zsend[ch, pl.ds(0, slots)]

    grad = query_part(0)
    for j in range(1, n_b):
        wait(qg_buf.at[j - 1], qg_rs.at[j - 1])
        grad = grad + qg_buf[j - 1].astype(f32)
    qg_ref[...] = grad.astype(bf16)

    wait(loss_m.at[pl.ds(0, n_mp - 1)], l_rs.at[1])
    loss_sum = jnp.sum(loss_m[...], axis=0)
    loss_ref[0, 0] = jnp.max(loss_sum) / (rows * n_batch * n_mp)

    for ch in range(n_ch):
        wait(zbuf.at[ch, pl.ds(slots, (n_mp - 1) * slots)], z_rs.at[ch])
        dg_ref[:, pl.ds(ch * cw, cw)] = dot(place[...], zbuf[ch]).astype(bf16)

    for j in range(1, n_b):
        wait(q_ref, q_ss.at[j - 1])
        wait(stat_own, s_ss.at[j - 1])
        wait(qg_send.at[j - 1], qg_ss.at[j - 1])
    for i in range(1, n_a):
        wait(d_ref, d_ss.at[i - 1])
        for ch in range(n_ch):
            wait(pg_send.at[i - 1, ch], pg_ss.at[i - 1, ch])
    wait(ids_buf, id_ss)
    for ch in range(n_ch):
        wait(zsend.at[ch, pl.ds(slots, (n_mp - 1) * slots)], z_ss.at[ch])
    wait(loss_b.at[pl.ds(0, n_batch - 1)], l_ss.at[0])
    wait(loss_m.at[pl.ds(0, n_mp - 1)], l_ss.at[1])


def place_outputs(qg_ref, dg_ref, qg_out, dg_out, sem):
    copies = [
        pltpu.make_async_copy(qg_ref, qg_out, sem.at[0]),
        pltpu.make_async_copy(dg_ref, dg_out, sem.at[1]),
    ]
    for copy in copies:
        copy.start()
    for copy in copies:
        copy.wait()


def per_device(n_batch, n_mp, queries, docs, doc_id, owner_row):
    rows, width = queries.shape
    own_rows = owner_row.shape[0]
    n_a = next(x for x in range(1, n_batch + 1) if n_batch % x == 0 and x * x >= n_batch)
    n_b = n_batch // n_a
    slots = max(16, -(-2 * rows // n_mp // 16) * 16)
    n_ch = max(1, width // 128)
    cw = width // n_ch
    vmem = pl.BlockSpec(memory_space=pltpu.VMEM)
    dma = pltpu.SemaphoreType.DMA
    ra, rb = max(n_a - 1, 1), max(n_b - 1, 1)
    query_grad, doc_grad, loss = pl.pallas_call(
        functools.partial(kernel, n_a, n_b, n_mp, slots, n_ch),
        out_shape=(
            jax.ShapeDtypeStruct((rows, width), bf16),
            jax.ShapeDtypeStruct((own_rows, width), bf16),
            jax.ShapeDtypeStruct((1, 1), f32),
        ),
        in_specs=[pl.BlockSpec(memory_space=pltpu.HBM)] * 4,
        out_specs=(vmem, vmem, pl.BlockSpec(memory_space=pltpu.SMEM)),
        scratch_shapes=[
            pltpu.VMEM((rb, rows, width), bf16),
            pltpu.VMEM((ra, rows, width), bf16),
            pltpu.VMEM((n_a, n_b, rows, rows), f32),
            pltpu.VMEM((n_a, n_b, rows, rows), bf16),
            pltpu.VMEM((2 * n_b, rows), f32),
            pltpu.VMEM((rb, 2 * n_b, rows), f32),
            pltpu.VMEM((rb, rows, width), bf16),
            pltpu.VMEM((rb, rows, width), bf16),
            pltpu.VMEM((ra, n_ch, rows, cw), bf16),
            pltpu.VMEM((ra, n_ch, rows, cw), bf16),
            pltpu.VMEM((n_ch, n_mp * slots, cw), bf16),
            pltpu.VMEM((n_ch, n_mp * slots, cw), bf16),
            pltpu.VMEM((n_mp - 1, 1, rows), jnp.int32),
            pltpu.VMEM((n_mp * slots, own_rows), f32),
            pltpu.VMEM((own_rows, n_mp * slots), bf16),
            pltpu.VMEM((n_mp * slots, 2 * rows), bf16),
            pltpu.VMEM((n_batch, 1, 128), f32),
            pltpu.VMEM((n_mp, 1, 128), f32),
            pltpu.VMEM((1, 128), f32),
            pltpu.VMEM((1, 128), f32),
            pltpu.VMEM((rows, width), bf16),
            pltpu.VMEM((rows, width), bf16),
            pltpu.VMEM((1, rows), jnp.int32),
            pltpu.VMEM((1, own_rows), jnp.int32),
            dma((rb,)), dma((rb,)), dma((ra,)), dma((ra,)), dma((rb,)), dma((rb,)),
            dma((rb,)), dma((rb,)), dma((ra, n_ch)), dma((ra, n_ch)),
            dma((n_ch,)), dma((n_ch,)), dma, dma, dma((2,)), dma((2,)), dma((4,)),
        ],
        compiler_params=pltpu.CompilerParams(
            collective_id=0, has_side_effects=True, vmem_limit_bytes=32 * 1024 * 1024
        ),
    )(queries, docs, doc_id.reshape(1, rows), owner_row.reshape(1, own_rows))
    hbm = pl.BlockSpec(memory_space=pl.ANY)
    query_grad, doc_grad = pl.pallas_call(
        place_outputs,
        out_shape=(
            jax.ShapeDtypeStruct((rows, width), bf16),
            jax.ShapeDtypeStruct((own_rows, width), bf16),
        ),
        in_specs=[vmem] * 2,
        out_specs=(hbm, hbm),
        scratch_shapes=[dma((2,))],
        compiler_params=pltpu.CompilerParams(vmem_limit_bytes=4 * 1024 * 1024),
    )(query_grad, doc_grad)
    return query_grad, doc_grad, loss.reshape(())


def solution(mesh):
    in_specs = (
        P(("batch", "mp"), None),
        P(("batch", "mp"), None),
        P(("batch", "mp")),
        P(("batch", "mp")),
    )
    out_specs = (P(("batch", "mp"), None), P(("batch", "mp"), None), P())
    body = functools.partial(per_device, mesh.shape["batch"], mesh.shape["mp"])
    return jax.shard_map(
        body, mesh=mesh, in_specs=in_specs, out_specs=out_specs, check_vma=False
    )
```

```python
import functools

import jax
import jax.numpy as jnp
from jax import lax
from jax.experimental import pallas as pl
from jax.experimental.pallas import tpu as pltpu
from jax.sharding import PartitionSpec as P

inverse_temp = 80.0
f32 = jnp.float32
bf16 = jnp.bfloat16
NT = (((1,), (1,)), ((), ()))
NN = (((1,), (0,)), ((), ()))
TN = (((0,), (0,)), ((), ()))


def dot(x, y, dims=NN):
    return lax.dot_general(x, y, dims, preferred_element_type=f32)


def iota(shape, dim):
    return lax.broadcasted_iota(jnp.int32, shape, dim)


def send(src, dst, send_sem, recv_sem, device):
    pltpu.make_async_remote_copy(
        src_ref=src,
        dst_ref=dst,
        send_sem=send_sem,
        recv_sem=recv_sem,
        device_id=device,
        device_id_type=pl.DeviceIdType.MESH,
    ).start()


def partner(m, k, n):
    if n & (n - 1):
        return (m + k) % n
    bit = 1
    while bit < n:
        if k & bit:
            m = m + bit * (1 - 2 * ((m // bit) % 2))
        bit *= 2
    return m


def wait(ref, sem):
    pltpu.make_async_copy(ref, ref, sem).wait()


def kernel(
    n_a, n_b, n_mp, slots, n_ch,
    q_hbm, d_hbm, id_hbm, own_hbm,
    qg_ref, dg_ref, loss_ref,
    qbuf, dbuf, st, gt, stat_own, stat_buf,
    qg_send, qg_buf, pg_send, pg_buf, zsend, zbuf,
    ids_buf, place_t, place, pick, loss_b, loss_m, loss_own, loss_grp,
    q_ref, d_ref, id_ref, own_ref,
    q_ss, q_rs, d_ss, d_rs, s_ss, s_rs, qg_ss, qg_rs, pg_ss, pg_rs,
    z_ss, z_rs, id_ss, id_rs, l_ss, l_rs, in_sem,
):
    rows, width = q_ref.shape
    own_rows = own_ref.shape[1]
    cw = width // n_ch
    n_batch = n_a * n_b
    me_b = lax.axis_index("batch")
    me_m = lax.axis_index("mp")
    a = me_b // n_b
    c = me_b % n_b

    def row_peer(j):
        return {"batch": a * n_b + (c + j) % n_b, "mp": me_m}

    def col_peer(i):
        return {"batch": ((a + i) % n_a) * n_b + c, "mp": me_m}

    def batch_peer(t):
        return {"batch": (me_b + t) % n_batch, "mp": me_m}

    def mp_peer(k):
        return {"batch": me_b, "mp": partner(me_m, k, n_mp)}

    load_q = pltpu.make_async_copy(q_hbm, q_ref, in_sem.at[0])
    load_d = pltpu.make_async_copy(d_hbm, d_ref, in_sem.at[1])
    load_id = pltpu.make_async_copy(id_hbm, id_ref, in_sem.at[2])
    load_own = pltpu.make_async_copy(own_hbm, own_ref, in_sem.at[3])
    loads = (load_q, load_d, load_id, load_own)
    for load in loads:
        load.start()

    barrier = pltpu.get_barrier_semaphore()
    for t in range(1, n_batch):
        pl.semaphore_signal(
            barrier, inc=1, device_id=batch_peer(t), device_id_type=pl.DeviceIdType.MESH
        )
    for k in range(1, n_mp):
        pl.semaphore_signal(
            barrier, inc=1, device_id=mp_peer(k), device_id_type=pl.DeviceIdType.MESH
        )
    pl.semaphore_wait(barrier, n_batch + n_mp - 2)
    for load in loads:
        load.wait()

    for j in range(1, n_b):
        to = n_b - j - 1
        send(q_ref, qbuf.at[to], q_ss.at[j - 1], q_rs.at[to], row_peer(j))
    for i in range(1, n_a):
        to = n_a - i - 1
        send(d_ref, dbuf.at[to], d_ss.at[i - 1], d_rs.at[to], col_peer(i))
    for k in range(1, n_mp):
        send(id_ref, ids_buf.at[k - 1], id_ss, id_rs, mp_peer(k))

    eye = iota((rows, rows), 0) == iota((rows, rows), 1)
    s00 = dot(d_ref[...], q_ref[...], NT) * inverse_temp
    st[0, 0] = s00
    own_score = jnp.sum(jnp.where(eye, s00, 0.0), axis=0, keepdims=True)

    upper = (iota((rows, rows), 0) < iota((rows, rows), 1)).astype(bf16)
    which = iota((n_mp, rows), 0)
    if n_mp & (n_mp - 1):
        col = me_m + which
        col = jnp.where(col >= n_mp, col - n_mp, col)
    else:
        col = jnp.broadcast_to(me_m, which.shape) ^ which
    first = (me_b * n_mp + col) * own_rows
    ids = jnp.broadcast_to(id_ref[...], (n_mp, rows))
    mask = ((ids >= first) & (ids < first + own_rows)).astype(f32)
    rank = dot(mask.astype(bf16), upper)
    count = jnp.sum(mask, axis=1, keepdims=True)
    first_slot = (which * slots).astype(f32)
    slot = jnp.sum(mask * (rank + first_slot), axis=0, keepdims=True)
    free = mask * (rank + count < slots).astype(f32)
    spare = jnp.sum(free * (rank + count + first_slot + 1.0), axis=0, keepdims=True) - 1.0
    at = iota((n_mp * slots, rows), 0)
    pick[:, pl.ds(0, rows)] = (at == slot.astype(jnp.int32)).astype(f32).astype(bf16)
    pick[:, pl.ds(rows, rows)] = (at == spare.astype(jnp.int32)).astype(f32).astype(bf16)

    base = (me_b * n_mp + me_m) * own_rows
    owner = (iota((own_rows, own_rows), 0) == own_ref[...] - base).astype(f32).astype(bf16)

    def place_block(k, ids_k):
        local = ids_k - base
        here = ((local >= 0) & (local < own_rows)).astype(f32)
        doc = (iota((own_rows, rows), 0) == local).astype(f32).astype(bf16)
        target = dot(owner, doc).astype(bf16)
        rank_k = dot(jnp.broadcast_to(here, (8, rows)).astype(bf16), upper)[0:1]
        spare_k = rank_k + jnp.sum(here, axis=1, keepdims=True)
        rank_k = jnp.where(here > 0.0, rank_k, -1.0).astype(jnp.int32)
        spare_k = jnp.where(here > 0.0, spare_k, -1.0).astype(jnp.int32)
        at_k = iota((slots, rows), 0)
        taken = ((at_k == rank_k) | (at_k == spare_k)).astype(f32).astype(bf16)
        place_t[pl.ds(k * slots, slots), :] = dot(taken, target, NT)

    place_block(0, id_ref[...])
    wait(ids_buf, id_rs)
    for k in range(1, n_mp):
        place_block(k, ids_buf[k - 1])
    place[...] = jnp.transpose(place_t[...]).astype(bf16)

    def q_of(j):
        return q_ref if j == 0 else qbuf.at[j - 1]

    def d_of(i):
        return d_ref if i == 0 else dbuf.at[i - 1]

    for i in range(1, n_a):
        wait(dbuf.at[i - 1], d_rs.at[i - 1])
        st[i, 0] = dot(d_of(i)[...], q_ref[...], NT) * inverse_temp
    for j in range(1, n_b):
        wait(qbuf.at[j - 1], q_rs.at[j - 1])
        for i in range(n_a):
            st[i, j] = dot(d_of(i)[...], q_of(j)[...], NT) * inverse_temp

    for j in range(n_b):
        top = jnp.max(st[0, j], axis=0, keepdims=True)
        for i in range(1, n_a):
            top = jnp.maximum(top, jnp.max(st[i, j], axis=0, keepdims=True))
        total = jnp.zeros_like(top)
        for i in range(n_a):
            e = jnp.exp(st[i, j] - top)
            st[i, j] = e
            total = total + jnp.sum(e, axis=0, keepdims=True)
        stat_own[pl.ds(2 * j, 1), :] = top
        stat_own[pl.ds(2 * j + 1, 1), :] = total
    for j in range(1, n_b):
        to = n_b - j - 1
        send(stat_own, stat_buf.at[to], s_ss.at[j - 1], s_rs.at[to], row_peer(j))
    for j in range(1, n_b):
        wait(stat_buf.at[j - 1], s_rs.at[j - 1])

    for j in range(n_b):
        tops = [stat_own[pl.ds(2 * j, 1), :]]
        totals = [stat_own[pl.ds(2 * j + 1, 1), :]]
        for s in range(1, n_b):
            r = (j - s) % n_b
            tops.append(stat_buf[s - 1, pl.ds(2 * r, 1), :])
            totals.append(stat_buf[s - 1, pl.ds(2 * r + 1, 1), :])
        top = functools.reduce(jnp.maximum, tops)
        total = sum(t * jnp.exp(m - top) for m, t in zip(tops, totals))
        scale = jnp.exp(tops[0] - top) / total
        if j == 0:
            part = jnp.sum(top + jnp.log(total) - own_score, axis=1, keepdims=True)
            loss_own[...] = jnp.broadcast_to(part, loss_own.shape)
            loss_b[me_b] = loss_own[...]
            for t in range(1, n_batch):
                send(loss_own, loss_b.at[me_b], l_ss.at[0], l_rs.at[0], batch_peer(t))
        for i in range(n_a):
            p = st[i, j] * scale
            if i == 0 and j == 0:
                p = p - eye.astype(f32)
            gt[i, j] = p.astype(bf16)

    def pair_part(i, ch):
        at = pl.ds(ch * cw, cw)
        return sum(dot(gt[i, j], q_of(j)[:, at]) for j in range(n_b)) * inverse_temp

    def query_part(j):
        return sum(dot(gt[i, j], d_of(i)[...], TN) for i in range(n_a)) * inverse_temp

    for ch in range(n_ch):
        for i in range(1, n_a):
            to = n_a - i - 1
            pg_send[i - 1, ch] = pair_part(i, ch).astype(bf16)
            send(
                pg_send.at[i - 1, ch], pg_buf.at[to, ch],
                pg_ss.at[i - 1, ch], pg_rs.at[to, ch], col_peer(i),
            )
    for j in range(1, n_b):
        to = n_b - j - 1
        qg_send[j - 1] = query_part(j).astype(bf16)
        send(qg_send.at[j - 1], qg_buf.at[to], qg_ss.at[j - 1], qg_rs.at[to], row_peer(j))

    wait(loss_b.at[pl.ds(0, n_batch - 1)], l_rs.at[0])
    loss_grp[...] = jnp.sum(loss_b[...], axis=0)
    for k in range(1, n_mp):
        send(loss_grp, loss_m.at[me_m], l_ss.at[1], l_rs.at[1], mp_peer(k))
    loss_m[me_m] = loss_grp[...]

    for ch in range(n_ch):
        part = pair_part(0, ch)
        for i in range(1, n_a):
            wait(pg_buf.at[i - 1, ch], pg_rs.at[i - 1, ch])
            part = part + pg_buf[i - 1, ch].astype(f32)
        high = part.astype(bf16)
        low = (part - high.astype(f32)).astype(bf16)
        zsend[ch] = dot(pick[...], jnp.concatenate([high, low], axis=0)).astype(bf16)
        for k in reversed(range(1, n_mp)):
            at = pl.ds(k * slots, slots)
            send(zsend.at[ch, at], zbuf.at[ch, at], z_ss.at[ch], z_rs.at[ch], mp_peer(k))
        zbuf[ch, pl.ds(0, slots)] = zsend[ch, pl.ds(0, slots)]

    grad = query_part(0)
    for j in range(1, n_b):
        wait(qg_buf.at[j - 1], qg_rs.at[j - 1])
        grad = grad + qg_buf[j - 1].astype(f32)
    qg_ref[...] = grad.astype(bf16)

    wait(loss_m.at[pl.ds(0, n_mp - 1)], l_rs.at[1])
    loss_sum = jnp.sum(loss_m[...], axis=0)
    loss_ref[0, 0] = jnp.max(loss_sum) / (rows * n_batch * n_mp)

    for ch in range(n_ch):
        wait(zbuf.at[ch, pl.ds(slots, (n_mp - 1) * slots)], z_rs.at[ch])
        dg_ref[:, pl.ds(ch * cw, cw)] = dot(place[...], zbuf[ch]).astype(bf16)

    for j in range(1, n_b):
        wait(q_ref, q_ss.at[j - 1])
        wait(stat_own, s_ss.at[j - 1])
        wait(qg_send.at[j - 1], qg_ss.at[j - 1])
    for i in range(1, n_a):
        wait(d_ref, d_ss.at[i - 1])
        for ch in range(n_ch):
            wait(pg_send.at[i - 1, ch], pg_ss.at[i - 1, ch])
    wait(ids_buf, id_ss)
    for ch in range(n_ch):
        wait(zsend.at[ch, pl.ds(slots, (n_mp - 1) * slots)], z_ss.at[ch])
    wait(loss_b.at[pl.ds(0, n_batch - 1)], l_ss.at[0])
    wait(loss_m.at[pl.ds(0, n_mp - 1)], l_ss.at[1])


def place_outputs(qg_ref, dg_ref, qg_out, dg_out, sem):
    copies = [
        pltpu.make_async_copy(qg_ref, qg_out, sem.at[0]),
        pltpu.make_async_copy(dg_ref, dg_out, sem.at[1]),
    ]
    for copy in copies:
        copy.start()
    for copy in copies:
        copy.wait()


def per_device(n_batch, n_mp, queries, docs, doc_id, owner_row):
    rows, width = queries.shape
    own_rows = owner_row.shape[0]
    n_a = next(x for x in range(1, n_batch + 1) if n_batch % x == 0 and x * x >= n_batch)
    n_b = n_batch // n_a
    slots = max(16, -(-2 * rows // n_mp // 16) * 16)
    n_ch = max(1, width // 128)
    cw = width // n_ch
    vmem = pl.BlockSpec(memory_space=pltpu.VMEM)
    dma = pltpu.SemaphoreType.DMA
    ra, rb = max(n_a - 1, 1), max(n_b - 1, 1)
    query_grad, doc_grad, loss = pl.pallas_call(
        functools.partial(kernel, n_a, n_b, n_mp, slots, n_ch),
        out_shape=(
            jax.ShapeDtypeStruct((rows, width), bf16),
            jax.ShapeDtypeStruct((own_rows, width), bf16),
            jax.ShapeDtypeStruct((1, 1), f32),
        ),
        in_specs=[pl.BlockSpec(memory_space=pltpu.HBM)] * 4,
        out_specs=(vmem, vmem, pl.BlockSpec(memory_space=pltpu.SMEM)),
        scratch_shapes=[
            pltpu.VMEM((rb, rows, width), bf16),
            pltpu.VMEM((ra, rows, width), bf16),
            pltpu.VMEM((n_a, n_b, rows, rows), f32),
            pltpu.VMEM((n_a, n_b, rows, rows), bf16),
            pltpu.VMEM((2 * n_b, rows), f32),
            pltpu.VMEM((rb, 2 * n_b, rows), f32),
            pltpu.VMEM((rb, rows, width), bf16),
            pltpu.VMEM((rb, rows, width), bf16),
            pltpu.VMEM((ra, n_ch, rows, cw), bf16),
            pltpu.VMEM((ra, n_ch, rows, cw), bf16),
            pltpu.VMEM((n_ch, n_mp * slots, cw), bf16),
            pltpu.VMEM((n_ch, n_mp * slots, cw), bf16),
            pltpu.VMEM((n_mp - 1, 1, rows), jnp.int32),
            pltpu.VMEM((n_mp * slots, own_rows), f32),
            pltpu.VMEM((own_rows, n_mp * slots), bf16),
            pltpu.VMEM((n_mp * slots, 2 * rows), bf16),
            pltpu.VMEM((n_batch, 1, 128), f32),
            pltpu.VMEM((n_mp, 1, 128), f32),
            pltpu.VMEM((1, 128), f32),
            pltpu.VMEM((1, 128), f32),
            pltpu.VMEM((rows, width), bf16),
            pltpu.VMEM((rows, width), bf16),
            pltpu.VMEM((1, rows), jnp.int32),
            pltpu.VMEM((1, own_rows), jnp.int32),
            dma((rb,)), dma((rb,)), dma((ra,)), dma((ra,)), dma((rb,)), dma((rb,)),
            dma((rb,)), dma((rb,)), dma((ra, n_ch)), dma((ra, n_ch)),
            dma((n_ch,)), dma((n_ch,)), dma, dma, dma((2,)), dma((2,)), dma((4,)),
        ],
        compiler_params=pltpu.CompilerParams(
            collective_id=0, has_side_effects=True, vmem_limit_bytes=32 * 1024 * 1024
        ),
    )(*(pltpu.with_memory_space_constraint(x, pltpu.HBM) for x in (queries, docs, doc_id.reshape(1, rows), owner_row.reshape(1, own_rows))))
    hbm = pl.BlockSpec(memory_space=pl.ANY)
    query_grad, doc_grad = pl.pallas_call(
        place_outputs,
        out_shape=(
            jax.ShapeDtypeStruct((rows, width), bf16),
            jax.ShapeDtypeStruct((own_rows, width), bf16),
        ),
        in_specs=[vmem] * 2,
        out_specs=(hbm, hbm),
        scratch_shapes=[dma((2,))],
        compiler_params=pltpu.CompilerParams(vmem_limit_bytes=4 * 1024 * 1024),
    )(query_grad, doc_grad)
    return query_grad, doc_grad, loss.reshape(())


def solution(mesh):
    in_specs = (
        P(("batch", "mp"), None),
        P(("batch", "mp"), None),
        P(("batch", "mp")),
        P(("batch", "mp")),
    )
    out_specs = (P(("batch", "mp"), None), P(("batch", "mp"), None), P())
    body = functools.partial(per_device, mesh.shape["batch"], mesh.shape["mp"])
    return jax.shard_map(
        body, mesh=mesh, in_specs=in_specs, out_specs=out_specs, check_vma=False
    )
```
